128 devices in a mesh: grp: 16 (over z_hi, y, core), tp: 8 (over x, z_lo).
Axes of the slice: x: 4, y: 4, z: 4 (z_hi: 2, z_lo: 2; z = z_hi * 2 + z_lo), core: 2. Of those that a mesh axis runs over, the one named last changes fastest.
Arguments:
- tokens: bfloat16 [8192, 6144], P('grp'), may hold values from -40 to 40
- norm_gain: bfloat16 [6144], replicated, may hold values from 0.099609375 to 1.8984375
- up_weight: bfloat16 [6144, 12288], P('grp', 'tp'), may hold values from -0.078125 to 0.078125
- up_bias: float32 [12288], P('tp'), may hold values from -3 to 3
- down_weight: bfloat16 [12288, 6144], P('tp', 'grp'), may hold values from -0.0546875 to 0.0546875
- down_bias: float32 [6144], P('tp'), may hold values from -2 to 2
Outputs:
- encoded: bfloat16 [8192, 6144], P('grp', 'tp')
The draws below stay inside these ranges and needn't reach their ends.
All inputs are finite; a program needn't handle non-finite values.
Results may differ from the reference program's by a relative error of at most 0.0085.
Values may be sent and summed in bfloat16 or wider, within the bound.
No kernel may reach another device: no remote copies, remote signals or barrier semaphores. Data moves between devices by JAX's collectives and lax.ppermute only.
A program may use at most 128 MiB of HBM per device.

```python
import jax
import jax.numpy as jnp
from jax import lax

D = 6144
FF = 12288
ROWS = 8192
N_TP = 8


def draw_tokens(key, part):
    keys = jax.random.split(key, 4)
    offsets = jax.random.uniform(keys[0], (16,), jnp.float32, -0.5, 0.5)
    column = jax.random.uniform(keys[1], (D,), jnp.float32, -0.5, 0.5) + jnp.repeat(offsets, D // 16)
    column_scale = 10.0 ** column
    row_scale = jnp.exp(jax.random.uniform(keys[2], (ROWS, 1), jnp.float32, -0.69, 0.69))
    base = jnp.clip(jax.random.normal(keys[3], (ROWS, D), jnp.float32), -6.0, 6.0)
    return jnp.clip(base * column_scale * row_scale, -40.0, 40.0).astype(jnp.bfloat16)


def block_scale(own_key, extent, pieces, low, largest):
    loudness, own = 1.0, jax.random.fold_in(own_key, 6)
    for dim, shards_of in pieces:
        steps = jnp.exp(jax.random.uniform(jax.random.fold_in(own, dim), (shards_of,), jnp.float32, low / len(pieces), largest / len(pieces)))
        loudness = loudness * jnp.repeat(steps, extent[dim] // shards_of).reshape([-1 if axis == dim else 1 for axis in range(len(extent))])
    return loudness


def bell_draw(rng, shape, spread, bound, shards=(), held_as=jnp.bfloat16):
    array = spread * jax.random.normal(rng, shape, jnp.float32)
    if shards:
        array = array * block_scale(rng, shape, shards, -0.22, 0.18)
    return jnp.clip(array, -bound, bound).astype(held_as)


def setup_inputs(seed: int = 0) -> dict:
    key_list = jax.random.split(jax.random.key(seed), 7)
    return {
        "tokens": draw_tokens(jax.random.fold_in(key_list[6], 71), 0),
        "norm_gain": jnp.clip(1.0 + 0.18 * jax.random.normal(key_list[1], (D,), jnp.float32), 0.099609375, 1.8984375).astype(jnp.bfloat16),
        "up_weight": bell_draw(key_list[2], (D, FF), D ** -0.5, 0.078125, ((0, 16), (1, 8))),
        "up_bias": bell_draw(key_list[3], (FF,), 0.5, 3.0, ((0, 8),), jnp.float32),
        "down_weight": bell_draw(key_list[4], (FF, D), FF ** -0.5, 0.0546875, ((0, 8), (1, 16))),
        "down_bias": bell_draw(key_list[5], (D,), 0.3, 2.0, ((0, 8),), jnp.float32),
    }


def reference(tokens, norm_gain, up_weight, up_bias, down_weight, down_bias):
    values = tokens.astype(jnp.float32)
    centre = lax.optimization_barrier(jnp.mean(values, axis=1, keepdims=True))
    shifted = values - centre
    variance = lax.optimization_barrier(jnp.mean(shifted * shifted, axis=1, keepdims=True))
    normed = (shifted * lax.rsqrt(variance + 1e-06) * norm_gain.astype(jnp.float32)).astype(jnp.bfloat16)
    pre = jnp.dot(normed, up_weight, preferred_element_type=jnp.float32) + up_bias
    hidden = jax.nn.gelu(pre, approximate=True).astype(jnp.bfloat16)
    width = FF // N_TP
    summed = jnp.zeros(values.shape, jnp.float32)
    for index in range(N_TP):
        term = jnp.dot(hidden[:, index * width:(index + 1) * width], down_weight[index * width:(index + 1) * width, :], preferred_element_type=jnp.float32)
        rounded = lax.optimization_barrier(term.astype(jnp.bfloat16))
        summed = summed + rounded.astype(jnp.float32)
    return (values + summed + down_bias).astype(jnp.bfloat16)
```

```python
import functools

import jax
import jax.numpy as jnp
from jax import lax
from jax.experimental import pallas as pl
from jax.experimental.pallas import tpu as pltpu
from jax.sharding import Mesh
from jax.sharding import PartitionSpec as P

GRP = ("zh", "y", "c")
TP = ("x", "zl")
F32 = jnp.float32
BF16 = jnp.bfloat16
LAG = 2
RS_LAG = 4
WIDE = 256
LANES = 128
TILE = 128
STEPS = (
    ("U0 +", "U0 -", "U0 z"),
    ("U1 +", "U1 -", "U1 z"),
    ("U0 2+", "U2 -", "U2 z"),
    ("U2 +", "U1z -", "U0- z"),
    ("U1z +", "U2z -", "U0+ z"),
    ("U1 2+", "U2 2-", "U02 z"),
    ("U2z +", "U2z 2-", "D0 z"),
    ("U1z 2+", "D2 -", "D1 z"),
    ("D2 +", "D0 -", "D2 z"),
    ("D0 +", "D2 2-", "D2- z"),
    ("D0z +", "D0z -", "D2+ z"),
    ("D1 +", "D0 2-", "D22 z"),
    ("D1z +", "D0z 2-", ""),
    ("D1 2+", "D1 -", ""),
    ("D1z 2+", "D1z -", ""),
)
UP_GROUPS = ((5, 4), (7, 6), (9, 8))


def shift(value, axis, step):
    n = lax.axis_size(axis)
    return lax.ppermute(value, axis, [(i, (i + step) % n) for i in range(n)])


def swap(value, axis):
    return shift(value, axis, 1)


def plan():
    moves, arrival = [], {}
    for number, entries in enumerate(STEPS):
        row = []
        for entry in entries:
            if not entry:
                continue
            source, how = entry.split()
            if how == "z":
                row.append((source, source[:2] + "z" + source[2:], "zh", 1))
            elif how[0] == "2":
                row.append((source + how[1], source + "2", "y", 1 if how[1] == "+" else -1))
            else:
                row.append((source, source + how, "y", 1 if how == "+" else -1))
        moves.append(row)
        for _, made, _, _ in row:
            arrival[made] = number + 1
    return moves, arrival


OFFSETS = {"": 0, "-": 1, "2": 2, "+": 3}


def place(name):
    far = name[2:3] == "z"
    return int(name[1]), 4 * far + OFFSETS[name[3:] if far else name[2:]]


def norm_kernel(order, source, gain, *refs):
    outs = refs[-3:]
    value = source[...].astype(F32)
    centre = jnp.mean(value, axis=1, keepdims=True)
    shifted = value - centre
    scale = lax.rsqrt(jnp.mean(shifted * shifted, axis=1, keepdims=True) + 1e-06)
    index = 0
    for out in outs:
        for start in range(0, out.shape[1], LANES):
            span = pl.ds(pl.multiple_of(order[index] * LANES, LANES), LANES)
            part = source[:, span].astype(F32) - centre
            out[:, start : start + LANES] = (part * scale * gain[:, span].astype(F32)).astype(BF16)
            index += 1


def normalise(order, source, gain, depths, filled):
    rows, width = source.shape
    tiles = rows // TILE
    base = tiles if filled else 0
    return pl.pallas_call(
        norm_kernel,
        out_shape=[jax.ShapeDtypeStruct((2 * rows, depth), BF16) for depth in depths],
        grid_spec=pltpu.PrefetchScalarGridSpec(
            num_scalar_prefetch=1,
            grid=(tiles,),
            in_specs=[
                pl.BlockSpec((TILE, width), lambda i, _: (i, 0)),
                pl.BlockSpec((1, width), lambda i, _: (0, 0)),
            ]
            + [pl.BlockSpec(memory_space=pl.ANY)] * len(filled),
            out_specs=[pl.BlockSpec((TILE, depth), lambda i, _: (base + i, 0)) for depth in depths],
        ),
        input_output_aliases={3 + i: i for i in range(len(filled))},
        cost_estimate=pl.CostEstimate(
            flops=8 * rows * width, bytes_accessed=4 * rows * width, transcendentals=0
        ),
    )(order, source, gain, *filled)


def up_kernel(final, count, values, start, *refs):
    parts, out, weight = refs[:count], refs[count], refs[count + 1]

    @pl.when(pl.program_id(0) == 0)
    def _():
        for index, part in enumerate(parts):
            weight[index * WIDE : (index + 1) * WIDE] = part[...]

    total = start[...] + jnp.dot(values[...], weight[...], preferred_element_type=F32)
    out[...] = jax.nn.gelu(total, approximate=True).astype(BF16) if final else total


def project_up(values, start, parts, final):
    rows, depth = values.shape
    width = parts[0].shape[1]
    tile = 2 * TILE
    return pl.pallas_call(
        functools.partial(up_kernel, final, len(parts)),
        out_shape=jax.ShapeDtypeStruct((rows, width), BF16 if final else F32),
        grid=(rows // tile,),
        in_specs=[
            pl.BlockSpec((tile, depth), lambda i: (i, 0)),
            pl.BlockSpec((1, width), lambda i: (0, 0))
            if start.shape[0] == 1
            else pl.BlockSpec((tile, width), lambda i: (i, 0)),
        ]
        + [pl.BlockSpec(memory_space=pltpu.VMEM)] * len(parts),
        out_specs=pl.BlockSpec((tile, width), lambda i: (i, 0)),
        scratch_shapes=[pltpu.VMEM((depth, width), BF16)],
        compiler_params=pltpu.CompilerParams(vmem_limit_bytes=36 << 20),
        cost_estimate=pl.CostEstimate(
            flops=2 * rows * depth * width,
            bytes_accessed=2 * rows * depth + 2 * depth * width + 8 * rows * width,
            transcendentals=0,
        ),
    )(values, start, *parts)


def down_kernel(slots, hidden, *refs):
    parts, (mine, other) = refs[:8], refs[8:]
    rows = mine.shape[1]
    for index, part in enumerate(parts):
        slot = slots[index]
        mine[slot] = jnp.dot(hidden[:rows], part[...], preferred_element_type=F32).astype(BF16)
        other[slot] = jnp.dot(hidden[rows:], part[...], preferred_element_type=F32).astype(BF16)


def project_down(slots, hidden, parts):
    rows = hidden.shape[0] // 2
    return pl.pallas_call(
        down_kernel,
        out_shape=[
            jax.ShapeDtypeStruct((8, rows, WIDE), BF16),
            jax.ShapeDtypeStruct((8, rows, WIDE), BF16),
        ],
        in_specs=[pl.BlockSpec(memory_space=pltpu.SMEM)]
        + [pl.BlockSpec(memory_space=pltpu.VMEM)] * 9,
        out_specs=[pl.BlockSpec(memory_space=pltpu.VMEM)] * 2,
        compiler_params=pltpu.CompilerParams(vmem_limit_bytes=24 << 20),
        cost_estimate=pl.CostEstimate(
            flops=2 * 2 * rows * hidden.shape[1] * 8 * WIDE,
            bytes_accessed=16 << 20,
            transcendentals=0,
        ),
    )(slots, hidden, *parts)


def per_device(tokens, norm_gain, up_weight, up_bias, down_weight, down_bias):
    rows, width = tokens.shape
    zh, y, core = lax.axis_index("zh"), lax.axis_index("y"), lax.axis_index("c")
    x, zl = lax.axis_index("x"), lax.axis_index("zl")
    half = up_weight.shape[1] // 2
    deep = 2 * up_weight.shape[0]
    moves, arrival = plan()

    def halves(value, dim):
        keep = lax.dynamic_slice_in_dim(value, core * half, half, dim)
        give = lax.dynamic_slice_in_dim(value, (1 - core) * half, half, dim)
        return keep, swap(give, "c")

    env = {}
    keep, got = halves(up_weight, 1)
    edge = up_weight.shape[0] - WIDE
    env["U0"] = keep[:WIDE]
    env["U1"] = jnp.concatenate([keep[WIDE:], got[: WIDE - edge]], 0)
    env["U2"] = got[WIDE - edge :]
    keep, got = halves(down_weight, 0)
    left, right = jnp.where(core == 0, keep, got), jnp.where(core == 0, got, keep)
    env["D0"] = left[:, :WIDE]
    env["D1"] = jnp.concatenate([left[:, WIDE:], right[:, : WIDE - edge]], 1)
    env["D2"] = right[:, WIDE - edge :]
    partner = swap(tokens, "c")

    own_width = down_bias.shape[0]
    own_start = (x * 2 + zl) * own_width
    base = lax.dynamic_slice_in_dim(tokens, own_start, own_width, 1).astype(F32) + down_bias
    bias = lax.dynamic_slice_in_dim(up_bias, core * half, half, 0)

    def chip(relative):
        return (zh ^ (relative // 4)) * 4 + (y + relative % 4) % 4

    def slot(block):
        return (block // 2 - x) % 4 * 2 + block % 2

    names = [f"{w}{i}{z}{o}" for w in "UD" for i in range(3) for z in ("", "z") for o in OFFSETS]
    ups = sorted((n for n in names if n[0] == "U"), key=lambda n: (arrival.get(n, 0), n))
    bounds = [sum(arrival.get(n, 0) <= last for n in ups) for _, last in UP_GROUPS]

    def lanes(name):
        chunk, relative = place(name)
        for block in (2 * chunk, 2 * chunk + 1):
            owner = core if block < 3 else 1 - core
            yield (chip(relative) * 2 + owner) * 3 + block % 3

    order = jnp.stack([lane for n in ups for lane in lanes(n)]).astype(jnp.int32)
    depths = [WIDE * (last - first) for first, last in zip([0] + bounds, bounds)]
    slots = jnp.stack([slot(chip(r)) for r in range(8)]).astype(jnp.int32)
    down_ready = {
        i: max(arrival.get(n, 0) for n in names if n[0] == "D" and int(n[1]) == i) for i in range(3)
    }
    gain = norm_gain.reshape(1, width)
    outs = {}
    live = {"partner": partner}
    for index, part in enumerate(normalise(order, tokens, gain, depths, [])):
        live[f"normed{index}"] = part
    live["pre"] = bias.reshape(1, half)

    def tie(keys, extra):
        everything = lax.optimization_barrier(
            ([env[k] for k in keys], [live[k] for k in extra])
        )
        env.update(zip(keys, everything[0]))
        live.update(zip(extra, everything[1]))

    made_at = {}
    for number in range(len(moves) + LAG + RS_LAG + 2):
        landed = [n for n, at in arrival.items() if at <= number - LAG + 1 and at > number - LAG]
        if number < len(moves):
            keys = sorted(set(landed) | {source for source, _, _, _ in moves[number]})
        else:
            keys = landed
        waiting = []
        for key in live:
            age = number - made_at.setdefault(key, number)
            if key[:-2] == "piece" and age < RS_LAG - 2:
                continue
            if key == "partner" and age < 2:
                continue
            waiting.append(key)
        if keys or waiting:
            tie(keys, waiting)
        if number < len(moves):
            for source, made, axis, step in moves[number]:
                env[made] = shift(env[source], axis, step)
        if number == 2:
            filled = [live[f"normed{index}"] for index in range(3)]
            filled = normalise(order, live.pop("partner"), gain, depths, filled)
            for index, part in enumerate(filled):
                live[f"normed{index}"] = part
        for index, (at, _) in enumerate(UP_GROUPS):
            if number == at:
                first, last = (bounds[index - 1] if index else 0), bounds[index]
                parts = [env[n] for n in ups[first:last]]
                final = index == len(UP_GROUPS) - 1
                live["hidden" if final else "pre"] = project_up(
                    live.pop(f"normed{index}"), live.pop("pre"), parts, final
                )
        for index in range(3):
            age = number - max(down_ready[index] + LAG - 1, UP_GROUPS[-1][0])
            if age == 0:
                parts = sorted((n for n in names if n[:2] == f"D{index}"), key=lambda n: place(n)[1])
                mine, other = project_down(slots, live["hidden"], [env[n] for n in parts])
                live[f"mine{index}"] = mine
                live[f"other{index}"] = swap(other, "c")
            if age == 1:
                total = live.pop(f"mine{index}").astype(F32) + live.pop(f"other{index}").astype(F32)
                live[f"acc{index}"] = total[:2]
                for step in (1, 3, 2):
                    piece = total[2 * step : 2 * step + 2].astype(BF16)
                    live[f"piece{index}{step}"] = shift(piece, "x", step)
            if age == RS_LAG:
                acc = live.pop(f"acc{index}")
                for step in (1, 3, 2):
                    acc = acc + live.pop(f"piece{index}{step}").astype(F32)
                live[f"keep{index}"] = lax.dynamic_index_in_dim(acc, zl, 0, keepdims=False)
                give = lax.dynamic_index_in_dim(acc, 1 - zl, 0, keepdims=False).astype(BF16)
                live[f"got{index}"] = swap(give, "zl")
            if age == RS_LAG + 1:
                span = slice(index * WIDE, (index + 1) * WIDE)
                value = live.pop(f"keep{index}") + live.pop(f"got{index}").astype(F32)
                outs[index] = (base[:, span] + value).astype(BF16)
    return jnp.concatenate([outs[i] for i in range(3)], 1)


def solution(mesh):
    split = Mesh(mesh.devices.reshape(2, 4, 2, 4, 2), ("zh", "y", "c", "x", "zl"))
    placed = (P(GRP, None), P(), P(GRP, TP), P(TP), P(TP, GRP), P(TP))
    return jax.shard_map(
        per_device, mesh=split, in_specs=placed, out_specs=P(GRP, TP), check_vma=False
    )
```
